32 devices in a mesh: dp: 4 (over x, core), ep: 8 (over z, y).
Axes of the slice: x: 2, y: 2, z: 4, core: 2. Of those that a mesh axis runs over, the one named last changes fastest.
Arguments:
- tokens: bfloat16 [4096, 2048], P(('dp', 'ep')), parts along dimension 0, may hold values from -6 to 6
- expert_ids: int32 [4096, 8], P(('dp', 'ep')), parts along dimension 0, may hold values from 0 to 15, all different within a row; in each aligned block of 32 rows (0 to 31, 32 to 63, ...) at most 32 rows name the same one
- gate_nums: int32 [4096, 8], P(('dp', 'ep')), parts along dimension 0, may hold values from 64 to 1023
- w_gate: bfloat16 [16, 2048, 768], P('ep'), may hold values from -0.125 to 0.125
- w_up: bfloat16 [16, 2048, 768], P('ep'), may hold values from -0.125 to 0.125
- w_down: bfloat16 [16, 768, 2048], P('ep'), may hold values from -0.21875 to 0.21875
Outputs:
- mixed: bfloat16 [4096, 2048], P(('dp', 'ep')), parts along dimension 0
The draws below stay inside these ranges and needn't reach their ends.
There are 4 independent parts, one for each index of `dp`. The reference program is written for one: setup_inputs(seed, part) draws one part's arguments, and reference() takes and returns one part's arrays. A program takes and returns all parts, laid end to end along the dimension named above; an argument that names none is the same for every part. Nothing has to cross between parts.
Inputs may be any that keep to these rules, and one draw needn't show every extreme that they name: `expert_ids`: each row names 8 different experts. In every aligned block of 32 rows no expert is named by more than 32 rows, a bound that some block reaches.
All inputs are finite; a program needn't handle non-finite values.
Results may differ from the reference program's by a relative error of at most 0.008.
Values may be sent and summed in bfloat16 or wider, within the bound.
A program may use at most 128 MiB of HBM per device.

```python
import math
import jax
import jax.numpy as jnp
import numpy as np
from jax import lax

D = 2048
FF = 768
TOP = 8
EXPERTS = 16
TOKENS = 1024
BLK = 32
CAP = 32


def touch_ends(array, own_key, least, high):
    extent = array.shape
    place = [jax.random.randint(jax.random.fold_in(own_key, axis), (), 0, extent[axis]) for axis in range(len(extent))]
    array = array.at[tuple(place)].set(least)
    longest = extent.index(max(extent))
    place[longest] = (place[longest] + 1) % extent[longest]
    return array.at[tuple(place)].set(high)


def steps_of(own_key, shape, split, low, largest):
    def one(axis_at, parts):
        steps = jax.random.uniform(jax.random.fold_in(jax.random.fold_in(own_key, 6), axis_at), (parts,), jnp.float32, low / len(split), largest / len(split))
        return jnp.repeat(jnp.exp(steps), shape[axis_at] // parts).reshape((-1,) + (1,) * (len(shape) - axis_at - 1))

    level = one(*split[0])
    for cut in split[1:]:
        level = level * one(*cut)
    return level


def deal_out(own_key, own, number, rows, count, top, most, lean):
    order = jax.random.permutation(own_key, count)
    heavy_load, ordinary = shares(count, rows * top, most, lean, True), shares(count, rows * top, most, lean, False)
    places = jnp.arange(count)

    def named(tallies, rotation):
        used = int((tallies > 0).sum())
        fixed = max(1, used // 4)
        moved = fixed + (places - fixed + rotation * (used - fixed)) % max(1, count - fixed)
        return jnp.zeros((count,), jnp.int32).at[order[jnp.where(places < fixed, places, moved)]].set(jnp.asarray(tallies, jnp.int32))

    tallies = jnp.where(number % 4 == 0, named(heavy_load, number // 4), named(ordinary, number - number // 4 - 1))
    mixed = jax.random.permutation(jax.random.fold_in(own, 3), count)
    source_of, sink = mixed[0:count // 2 * 2:2], mixed[1:count // 2 * 2:2]
    margin = jnp.minimum(tallies[source_of] - 1, most - tallies[sink]) // 2
    margin = jnp.where((source_of == order[0]) | (sink == order[0]) | (tallies[sink] == 0), 0, jnp.maximum(margin, 0))
    moved = jax.random.randint(jax.random.fold_in(own, 4), (count // 2,), 0, 1 << 20) % (margin + 1)
    tallies = tallies.at[source_of].add(-moved).at[sink].add(moved)
    members = jnp.searchsorted(jnp.cumsum(tallies), jnp.arange(rows * top), side="right").astype(jnp.int32)
    table = members.reshape(top, rows).T
    table = table[jax.random.permutation(jax.random.fold_in(own, 1), rows)]
    rotation = jax.random.randint(jax.random.fold_in(own, 2), (rows, 1), 0, top)
    return jnp.take_along_axis(table, (jnp.arange(top)[None, :] + rotation) % top, axis=1)


def shares(amount, total, bound, lean, full):
    loads = [(1 << 20) // math.isqrt(rank ** lean) + 1 for rank in range(1, amount + 1)]
    largest = bound if full else min(bound, max(-(-total // amount), total * loads[0] // sum(loads)))
    least = 1 if total - largest >= amount - 1 else 0
    holding, surplus = [largest] + [least] * (amount - 1), total - largest - least * (amount - 1)
    while surplus > 0:
        movable = [i for i in range(1, amount) if holding[i] < largest] or [i for i in range(1, amount) if holding[i] < bound]
        mass, budget = sum([loads[i] for i in movable]), surplus
        for i in movable:
            addition = min(bound - holding[i], max(1, budget * loads[i] // mass), surplus)
            holding[i] = holding[i] + addition
            surplus = surplus - addition
    return np.array(holding)


def noise(rng, extent, deviation, limit, shards=(), held_as=jnp.bfloat16):
    entries = deviation * jax.random.normal(rng, extent, jnp.float32)
    if shards:
        entries = entries * steps_of(rng, extent, shards, -0.22, 0.18)
    return jnp.clip(entries, -limit, limit).astype(held_as)


def setup_inputs(seed: int = 0, part: int = 0) -> dict:
    keys = jax.random.split(jax.random.key(seed), 7)
    part_keys = jax.random.split(jax.random.fold_in(keys[6], part), 7)
    tokens = noise(part_keys[0], (TOKENS, D), 1.0, 6.0, ((0, 8),))
    expert_ids_keys = jax.random.split(jax.random.fold_in(part_keys[1], 1), TOKENS // BLK)
    expert_ids_turns = jax.random.permutation(jax.random.fold_in(part_keys[1], 3), TOKENS // BLK)
    expert_ids = jax.vmap(lambda own, number: deal_out(jax.random.fold_in(part_keys[1], 2), own, number, BLK, EXPERTS, TOP, CAP, 2))(expert_ids_keys, expert_ids_turns).reshape((TOKENS, TOP))
    gate_nums = touch_ends(jax.random.randint(part_keys[2], (TOKENS, TOP), 64, 1024), jax.random.fold_in(part_keys[2], 1), 64, 1023).astype(jnp.int32)
    w_gate = noise(keys[3], (EXPERTS, D, FF), D ** -0.5, 0.125, ((0, 8),))
    w_up = noise(keys[4], (EXPERTS, D, FF), D ** -0.5, 0.125, ((0, 8),))
    w_down = noise(keys[5], (EXPERTS, FF, D), FF ** -0.5, 0.21875, ((0, 8),))
    return {"tokens": tokens, "expert_ids": expert_ids, "gate_nums": gate_nums, "w_gate": w_gate, "w_up": w_up, "w_down": w_down}


denominator = 1024.0


def reference(tokens, expert_ids, gate_nums, w_gate, w_up, w_down):
    total = tokens.shape[0]
    most = CAP * (total // BLK)
    gates = gate_nums.astype(jnp.float32) / denominator

    def step(accum, expert):
        hit = expert_ids == expert
        weight = jnp.sum(jnp.where(hit, gates, jnp.zeros_like(gates)), axis=1)
        member = jnp.any(hit, axis=1)
        index = jnp.nonzero(member, size=most, fill_value=0)[0].astype(jnp.int32)
        valid = jnp.arange(most, dtype=jnp.int32) < jnp.sum(member.astype(jnp.int32))
        picked = tokens[index]
        gate = jnp.dot(picked, w_gate[expert], preferred_element_type=jnp.float32)
        up = jnp.dot(picked, w_up[expert], preferred_element_type=jnp.float32)
        hidden = (jax.nn.silu(gate) * up).astype(jnp.bfloat16)
        result = jnp.dot(hidden, w_down[expert], preferred_element_type=jnp.float32).astype(jnp.bfloat16)
        scale = jnp.where(valid, weight[index], jnp.zeros_like(weight[index]))
        accum = accum.at[index].add(scale[:, None] * result.astype(jnp.float32))
        return accum, None

    start = jnp.zeros((total, tokens.shape[1]), jnp.float32)
    accum, _ = lax.scan(step, start, jnp.arange(EXPERTS, dtype=jnp.int32))
    return accum.astype(jnp.bfloat16)
```

```python
import jax
import jax.numpy as jnp
from jax import lax
from jax.sharding import PartitionSpec as P

denominator = 1024.0


def shards(tokens, expert_ids, gate_nums, w_gate, w_up, w_down):
    ways = lax.axis_size("ep")
    local = w_gate.shape[0]
    experts = local * ways
    gates = gate_nums.astype(jnp.float32) / denominator
    labels = jnp.arange(experts, dtype=jnp.int32)
    onehot = expert_ids[:, :, None] == labels[None, None, :]
    weight = jnp.sum(jnp.where(onehot, gates[:, :, None], 0.0), axis=1)
    weights = lax.all_to_all(weight, "ep", split_axis=1, concat_axis=0, tiled=True)
    rows = lax.all_gather(tokens, "ep", axis=0, tiled=True)
    gate = jnp.einsum("td,xdf->xtf", rows, w_gate, preferred_element_type=jnp.float32)
    up = jnp.einsum("td,xdf->xtf", rows, w_up, preferred_element_type=jnp.float32)
    hidden = (jax.nn.silu(gate) * up * weights.T[:, :, None]).astype(jnp.bfloat16)
    result = jnp.einsum("xtf,xfd->td", hidden, w_down, preferred_element_type=jnp.float32)
    return lax.psum_scatter(
        result.astype(jnp.bfloat16), "ep", scatter_dimension=0, tiled=True
    )


def solution(mesh):
    placed = (
        P(("dp", "ep"), None),
        P(("dp", "ep"), None),
        P(("dp", "ep"), None),
        P("ep", None, None),
        P("ep", None, None),
        P("ep", None, None),
    )
    return jax.shard_map(
        shards, mesh=mesh, in_specs=placed, out_specs=P(("dp", "ep"), None), check_vma=False
    )
```

```python
import functools

import jax
import jax.numpy as jnp
from jax import lax
from jax.experimental import pallas as pl
from jax.experimental.pallas import tpu as pltpu
from jax.sharding import PartitionSpec as P

denominator = 1024.0
SIDE = 2
LANES = 256
VMEM = 60 * 2**20


def expert_weights(expert_ids, gate_nums, experts):
    gates = gate_nums.astype(jnp.float32) / denominator
    labels = jnp.arange(experts, dtype=jnp.int32)
    onehot = expert_ids[:, :, None] == labels[None, None, :]
    return jnp.sum(jnp.where(onehot, gates[:, :, None], 0.0), axis=1)


def kernel(
    n, local,
    tokens, weights, w_gate, w_up, w_down, out,
    rows, factors, gate, up, down, hidden, part, from_side, from_line,
    load_sem, weight_send, weight_recv, line_send, line_recv, side_send, side_recv,
    back_side_send, back_side_recv, back_line_send, back_line_recv,
):
    depth = n // SIDE
    me = lax.axis_index("ep")
    z, y = me // SIDE, me % SIDE
    partner = z * SIDE + (SIDE - 1 - y)
    other = SIDE - 1 - y
    ff = w_gate.shape[2]
    count = tokens.shape[0]
    width = tokens.shape[1]

    def remote(source, target, send, recv, device):
        return pltpu.make_async_remote_copy(
            src_ref=source, dst_ref=target, send_sem=send, recv_sem=recv,
            device_id={"ep": device}, device_id_type=pl.DeviceIdType.MESH,
        )

    own = pltpu.make_async_copy(tokens, rows.at[z, y], load_sem.at[0])
    own.start()
    loads = []
    for e in range(local):
        cut = pl.ds(e * ff, ff)
        loads.append(pltpu.make_async_copy(w_gate.at[e], gate.at[e], load_sem.at[1 + 3 * e]))
        loads.append(pltpu.make_async_copy(w_up.at[e], up.at[e], load_sem.at[2 + 3 * e]))
        loads.append(pltpu.make_async_copy(w_down.at[e], down.at[cut], load_sem.at[3 + 3 * e]))
    for load in loads:
        load.start()

    barrier = pltpu.get_barrier_semaphore()
    for k in range(1, n):
        pl.semaphore_signal(
            barrier, inc=1, device_id={"ep": (me + k) % n}, device_id_type=pl.DeviceIdType.MESH
        )
    pl.semaphore_wait(barrier, n - 1)

    own.wait()

    def side_copy(o):
        return remote(rows.at[o, y], rows.at[o, y], side_send.at[o], side_recv.at[o], partner)

    def line_copy(k):
        there = ((z + k) % depth) * SIDE + y
        return remote(rows.at[z, y], rows.at[z, y], line_send.at[k], line_recv.at[z], there)

    def weight_copy(k):
        there = (me + k) % n
        return remote(weights.at[there], factors.at[me], weight_send.at[k], weight_recv.at[me], there)

    def part_copy(o):
        return remote(
            part.at[o, other], from_side.at[o], back_side_send.at[o], back_side_recv.at[o], partner
        )

    def sum_copy(o):
        there = o * SIDE + y
        return remote(
            part.at[o, y], from_line.at[z], back_line_send.at[o], back_line_recv.at[z], there
        )

    side_copy(z).start()
    for k in range(1, n):
        weight_copy(k).start()
    for k in range(1, depth):
        line_copy(k).start()
    factors[me] = weights[me]
    for load in loads:
        load.wait()
    for k in range(1, n):
        source = (me + k) % n
        remote(
            factors.at[source], factors.at[source], weight_send.at[k], weight_recv.at[source], partner
        ).wait_recv()

    turn = 1 - 2 * (z // (depth // 2))

    def origin(s):
        return (z + turn * s + depth) % depth

    def gather_next(o):
        remote(
            rows.at[o, y], rows.at[o, y], line_send.at[0], line_recv.at[o], partner
        ).wait_recv()
        side_copy(o).start()

    def finish(o):
        remote(
            from_side.at[o], from_side.at[o], back_side_send.at[o], back_side_recv.at[o], partner
        ).wait_recv()

    def pass_back(o):
        finish(o)
        total = part[o, y].astype(jnp.float32) + from_side[o].astype(jnp.float32)
        part[o, y] = total.astype(jnp.bfloat16)
        sum_copy(o).start()

    def step(s, carry):
        o = origin(s)
        remote(
            rows.at[o, other], rows.at[o, other], side_send.at[o], side_recv.at[o], partner
        ).wait_recv()
        scale = jnp.concatenate([factors[o * SIDE + i].T for i in range(SIDE)], axis=0)
        for e in range(local):
            column = scale[:, e : e + 1]

            def tile(t, carry):
                cut = pl.ds(pl.multiple_of(t * LANES, LANES), LANES)
                block = rows[o].reshape(SIDE * count, width)
                g = jnp.dot(block, gate[e, :, cut], preferred_element_type=jnp.float32)
                u = jnp.dot(block, up[e, :, cut], preferred_element_type=jnp.float32)
                h = g / (1.0 + jnp.exp(-g)) * u * column
                place = pl.ds(pl.multiple_of(e * ff + t * LANES, LANES), LANES)
                hidden[:, place] = h.astype(jnp.bfloat16)
                return carry

            lax.fori_loop(0, ff // LANES, tile, 0)

        @pl.when(s + 1 < depth)
        def _():
            gather_next(origin(s + 1))

        def spread(t, carry):
            cut = pl.ds(pl.multiple_of(t * LANES, LANES), LANES)
            result = jnp.dot(hidden[...], down[:, cut], preferred_element_type=jnp.float32)
            part[o, :, :, cut] = result.astype(jnp.bfloat16).reshape(SIDE, count, LANES)
            return carry

        lax.fori_loop(0, width // LANES, spread, 0)
        part_copy(o).start()

        @pl.when(s >= 2)
        def _():
            pass_back(origin(s - 1))

        return carry

    lax.fori_loop(0, depth, step, 0)
    if depth > 1:
        pass_back(origin(depth - 1))
    finish(z)
    total = part[z, y].astype(jnp.float32) + from_side[z].astype(jnp.float32)
    for s in range(1, depth):
        o = origin(s)
        remote(
            from_line.at[o], from_line.at[o], back_line_send.at[o], back_line_recv.at[o], partner
        ).wait_recv()
        total = total + from_line[o].astype(jnp.float32)
    out[...] = total.astype(jnp.bfloat16)
    for k in range(1, n):
        weight_copy(k).wait_send()
    for k in range(1, depth):
        line_copy(k).wait_send()
    for o in range(depth):
        side_copy(o).wait_send()
        part_copy(o).wait_send()
    for k in range(1, depth):
        sum_copy((z + k) % depth).wait_send()


def fused(tokens, expert_ids, gate_nums, w_gate, w_up, w_down, n):
    count, width = tokens.shape
    local, _, ff = w_gate.shape
    depth = n // SIDE
    weight = expert_weights(expert_ids, gate_nums, local * n)
    pad = -local % 8
    weights = jnp.pad(weight.T.reshape(n, local, count), ((0, 0), (0, pad), (0, 0)))
    kind = tokens.dtype
    dma = pltpu.SemaphoreType.DMA
    vmem = pl.BlockSpec(memory_space=pltpu.VMEM)
    hbm = pl.BlockSpec(memory_space=pl.ANY)
    return pl.pallas_call(
        functools.partial(kernel, n, local),
        out_shape=jax.ShapeDtypeStruct((count, width), kind),
        in_specs=[hbm, vmem, hbm, hbm, hbm],
        out_specs=vmem,
        scratch_shapes=[
            pltpu.VMEM((depth, SIDE, count, width), kind),
            pltpu.VMEM((n, local + pad, count), jnp.float32),
            pltpu.VMEM((local, width, ff), kind),
            pltpu.VMEM((local, width, ff), kind),
            pltpu.VMEM((local * ff, width), kind),
            pltpu.VMEM((SIDE * count, local * ff), kind),
            pltpu.VMEM((depth, SIDE, count, width), kind),
            pltpu.VMEM((depth, count, width), kind),
            pltpu.VMEM((depth, count, width), kind),
            dma((1 + 3 * local,)),
            dma((n,)), dma((n,)),
            dma((depth,)), dma((depth,)),
            dma((depth,)), dma((depth,)),
            dma((depth,)), dma((depth,)),
            dma((depth,)), dma((depth,)),
        ],
        compiler_params=pltpu.CompilerParams(
            collective_id=0, has_side_effects=True, vmem_limit_bytes=VMEM
        ),
    )(tokens, weights, w_gate, w_up, w_down)


def plain(tokens, expert_ids, gate_nums, w_gate, w_up, w_down, n):
    weight = expert_weights(expert_ids, gate_nums, w_gate.shape[0] * n)
    weights = lax.all_to_all(weight, "ep", split_axis=1, concat_axis=0, tiled=True)
    rows = lax.all_gather(tokens, "ep", axis=0, tiled=True)
    gate = jnp.einsum("td,xdf->xtf", rows, w_gate, preferred_element_type=jnp.float32)
    up = jnp.einsum("td,xdf->xtf", rows, w_up, preferred_element_type=jnp.float32)
    hidden = (jax.nn.silu(gate) * up * weights.T[:, :, None]).astype(jnp.bfloat16)
    result = jnp.einsum("xtf,xfd->td", hidden, w_down, preferred_element_type=jnp.float32)
    return lax.psum_scatter(
        result.astype(jnp.bfloat16), "ep", scatter_dimension=0, tiled=True
    )


def shards(n, tokens, expert_ids, gate_nums, w_gate, w_up, w_down):
    count, width = tokens.shape
    local, _, ff = w_gate.shape
    held = 3 * n * count * width + 3 * local * width * ff + 2 * count * local * ff
    fits = 2 * held < VMEM - 4 * 2**20
    shaped = n % (2 * SIDE) == 0 and count % 128 == 0 and ff % LANES == 0 and width % LANES == 0
    plan = fused if fits and shaped else plain
    return plan(tokens, expert_ids, gate_nums, w_gate, w_up, w_down, n)


def solution(mesh):
    placed = (
        P(("dp", "ep"), None),
        P(("dp", "ep"), None),
        P(("dp", "ep"), None),
        P("ep", None, None),
        P("ep", None, None),
        P("ep", None, None),
    )
    return jax.shard_map(
        functools.partial(shards, mesh.shape["ep"]),
        mesh=mesh, in_specs=placed, out_specs=P(("dp", "ep"), None), check_vma=False,
    )
```

```python
import functools

import jax
import jax.numpy as jnp
from jax import lax
from jax.experimental import pallas as pl
from jax.experimental.pallas import tpu as pltpu
from jax.sharding import PartitionSpec as P

denominator = 1024.0
SIDE = 2
LANES = 256
VMEM = 60 * 2**20


def expert_weights(expert_ids, gate_nums, experts):
    gates = gate_nums.astype(jnp.float32) / denominator
    labels = jnp.arange(experts, dtype=jnp.int32)
    onehot = expert_ids[:, :, None] == labels[None, None, :]
    return jnp.sum(jnp.where(onehot, gates[:, :, None], 0.0), axis=1)


def kernel(
    n, local, messages,
    tokens, weights, w_gate, w_up, w_down, out,
    rows, factors, gate, up, down, hidden, part, from_side, from_line,
    load_sem, weight_send, weight_recv, line_send, line_recv, side_send, side_recv,
    back_side_send, back_side_recv, back_line_send, back_line_recv,
):
    depth = n // SIDE
    me = lax.axis_index("ep")
    z, y = me // SIDE, me % SIDE
    other = SIDE - 1 - y
    partner = z * SIDE + other
    ff = w_gate.shape[2]
    count = tokens.shape[0]
    width = tokens.shape[1]
    last = depth - 1
    late = [m for m, (_, _, first) in enumerate(messages) if not first]
    early = [m for m, (_, _, first) in enumerate(messages) if first]
    cuts = [pl.ds(start, size) for start, size, _ in messages]

    def remote(source, target, send, recv, device):
        return pltpu.make_async_remote_copy(
            src_ref=source, dst_ref=target, send_sem=send, recv_sem=recv,
            device_id={"ep": device}, device_id_type=pl.DeviceIdType.MESH,
        )

    own = pltpu.make_async_copy(tokens, rows.at[z, y], load_sem.at[0])
    own.start()
    loads = []
    for e in range(local):
        cut = pl.ds(e * ff, ff)
        loads.append(pltpu.make_async_copy(w_gate.at[e], gate.at[e], load_sem.at[1 + 3 * e]))
        loads.append(pltpu.make_async_copy(w_up.at[e], up.at[e], load_sem.at[2 + 3 * e]))
        loads.append(pltpu.make_async_copy(w_down.at[e], down.at[cut], load_sem.at[3 + 3 * e]))
    for load in loads:
        load.start()

    barrier = pltpu.get_barrier_semaphore()
    for k in range(1, n):
        pl.semaphore_signal(
            barrier, inc=1, device_id={"ep": (me + k) % n}, device_id_type=pl.DeviceIdType.MESH
        )
    pl.semaphore_wait(barrier, n - 1)
    own.wait()

    def side_copy(o, row, m):
        ref = rows.at[o, row, cuts[m]]
        return remote(ref, ref, side_send.at[o, m], side_recv.at[o, m], partner)

    def line_copy(o, row, m, way):
        ref = rows.at[o, row, cuts[m]]
        there = me + SIDE * (1 - 2 * way)
        return remote(
            ref, ref, line_send.at[way, o, row, m], line_recv.at[o, row, m], there
        )

    def onward(o, row, m, act):
        @pl.when((o <= z) & (z < last))
        def _():
            act(line_copy(o, row, m, 0))

        @pl.when((o >= z) & (z > 0))
        def _():
            act(line_copy(o, row, m, 1))

    def start(copy):
        copy.start()

    def wait_send(copy):
        copy.wait_send()

    def weight_copy(k):
        there = (me + k) % n
        return remote(weights.at[there], factors.at[me], weight_send.at[k], weight_recv.at[me], there)

    def back_side(o, m):
        return remote(
            part.at[o, other, cuts[m]], from_side.at[o, cuts[m]],
            back_side_send.at[o, m], back_side_recv.at[o, m], partner,
        )

    def back_line(o, row, m, way):
        there = me + SIDE * (1 - 2 * way)
        return remote(
            part.at[o, row, cuts[m]], from_line.at[way, o, row, cuts[m]],
            back_line_send.at[o, row, m], back_line_recv.at[way, o, row, m], there,
        )

    def each_back(o, row, m, act):
        @pl.when(o > z)
        def _():
            act(back_line(o, row, m, 0))

        @pl.when(o < z)
        def _():
            act(back_line(o, row, m, 1))

    for m in early:
        side_copy(z, y, m).start()
    for k in range(1, n):
        weight_copy(k).start()
    for m in late:
        onward(z, y, m, start)
        side_copy(z, y, m).start()
    for m in early:
        onward(z, y, m, start)
    factors[me] = weights[me]

    @pl.when(z == 0)
    def _():
        from_line[0] = jnp.zeros_like(from_line[0])

    @pl.when(z == last)
    def _():
        from_line[1] = jnp.zeros_like(from_line[1])

    for m in early:
        side_copy(z, other, m).wait_recv()
        onward(z, other, m, start)

    turn = 1 - 2 * (z // (depth // 2))
    pairs = jnp.minimum(z, last - z)
    middle = jnp.minimum(pairs, 1)

    def nearest(s):
        both = z + turn * ((s + 1) // 2) * (2 * (s % 2) - 1)
        single = z + turn * (s - pairs)
        return jnp.where(s <= 2 * pairs, both, single)

    def rotation(s):
        return (z + turn * s + depth) % depth

    def gather(o):
        for m in late:
            line_copy(o, y, m, 0).wait_recv()
            onward(o, y, m, start)
            side_copy(o, y, m).start()
        for m in early:
            for row in range(SIDE):
                line_copy(o, row, m, 0).wait_recv()
                onward(o, row, m, start)

    gather(nearest(1))

    @pl.when(middle == 1)
    def _():
        gather(nearest(2))

    for load in loads:
        load.wait()
    for k in range(1, n):
        source = (me + k) % n
        remote(
            factors.at[source], factors.at[source], weight_send.at[k], weight_recv.at[source], partner
        ).wait_recv()

    def arrive(o, row, m):
        @pl.when((o >= z) & (z > 0))
        def _():
            back_line(o, row, m, 0).wait_recv()

        @pl.when((o <= z) & (z < last))
        def _():
            back_line(o, row, m, 1).wait_recv()

    def wide(ref):
        return ref[...].astype(jnp.float32)

    def pass_back(o):
        way = (last + z - o) // depth
        for m in early:
            for row in range(SIDE):
                arrive(o, row, m)
                total = wide(part.at[o, row, cuts[m]]) + wide(from_line.at[way, o, row, cuts[m]])
                part[o, row, cuts[m]] = total.astype(part.dtype)
                each_back(o, row, m, start)
        for m in late:
            back_side(o, m).wait_recv()
            arrive(o, y, m)
            total = wide(part.at[o, y, cuts[m]]) + wide(from_line.at[way, o, y, cuts[m]])
            total = total + wide(from_side.at[o, cuts[m]])
            part[o, y, cuts[m]] = total.astype(part.dtype)
            each_back(o, y, m, start)

    def step(s, carry):
        o = nearest(s)
        for m in late:
            side_copy(o, other, m).wait_recv()
        scale = jnp.concatenate([factors[o * SIDE + i].T for i in range(SIDE)], axis=0)
        for e in range(local):
            column = scale[:, e : e + 1]

            def tile(t, carry):
                cut = pl.ds(pl.multiple_of(t * LANES, LANES), LANES)
                block = rows[o].reshape(SIDE * count, width)
                g = jnp.dot(block, gate[e, :, cut], preferred_element_type=jnp.float32)
                u = jnp.dot(block, up[e, :, cut], preferred_element_type=jnp.float32)
                h = g / (1.0 + jnp.exp(-g)) * u * column
                place = pl.ds(pl.multiple_of(e * ff + t * LANES, LANES), LANES)
                hidden[:, place] = h.astype(jnp.bfloat16)
                return carry

            lax.fori_loop(0, ff // LANES, tile, 0)

        def spread(t, carry):
            cut = pl.ds(pl.multiple_of(t * LANES, LANES), LANES)
            result = jnp.dot(hidden[...], down[:, cut], preferred_element_type=jnp.float32)
            part[o, :, :, cut] = result.astype(jnp.bfloat16).reshape(SIDE, count, LANES)
            return carry

        lax.fori_loop(0, width // LANES, spread, 0)

        @pl.when(s + 2 + middle < depth)
        def _():
            gather(nearest(s + 2 + middle))

        @pl.when(s > 0)
        def _():
            for m in late:
                back_side(o, m).start()

        @pl.when((s >= 2) & (middle == 0))
        def _():
            pass_back(rotation(s - 1))

        return carry

    lax.fori_loop(0, depth, step, 0)
    for m in late:
        back_side(z, m).start()

    def rest(s, carry):
        pass_back(rotation(s))
        return carry

    lax.fori_loop(1 + (1 - middle) * (depth - 2), depth, rest, 0)

    def collected(row, m):
        arrive(z, row, m)
        total = wide(part.at[z, row, cuts[m]])
        return total + wide(from_line.at[0, z, row, cuts[m]]) + wide(from_line.at[1, z, row, cuts[m]])

    for m in early:
        part[z, other, cuts[m]] = collected(other, m).astype(part.dtype)
        back_side(z, m).start()
    for m in late + early:
        total = collected(y, m)
        back_side(z, m).wait_recv()
        out[cuts[m]] = (total + wide(from_side.at[z, cuts[m]])).astype(out.dtype)

    for k in range(1, n):
        weight_copy(k).wait_send()
    for m in early:
        side_copy(z, y, m).wait_send()
        back_side(z, m).wait_send()

    def settle(o, carry):
        for m in late:
            side_copy(o, y, m).wait_send()
            back_side(o, m).wait_send()
            onward(o, y, m, wait_send)
            each_back(o, y, m, wait_send)
        for m in early:
            for row in range(SIDE):
                onward(o, row, m, wait_send)
                each_back(o, row, m, wait_send)
        return carry

    lax.fori_loop(0, depth, settle, 0)


def fused(tokens, expert_ids, gate_nums, w_gate, w_up, w_down, n):
    count, width = tokens.shape
    local, _, ff = w_gate.shape
    depth = n // SIDE
    weight = expert_weights(expert_ids, gate_nums, local * n)
    pad = -local % 8
    weights = jnp.pad(weight.T.reshape(n, local, count), ((0, 0), (0, pad), (0, 0)))
    unit = count // 8
    messages = [(0, 3 * unit, False), (3 * unit, 3 * unit, False), (6 * unit, 2 * unit, True)]
    size = len(messages)
    kind = tokens.dtype
    dma = pltpu.SemaphoreType.DMA
    vmem = pl.BlockSpec(memory_space=pltpu.VMEM)
    hbm = pl.BlockSpec(memory_space=pl.ANY)
    return pl.pallas_call(
        functools.partial(kernel, n, local, messages),
        out_shape=jax.ShapeDtypeStruct((count, width), kind),
        in_specs=[hbm, vmem, hbm, hbm, hbm],
        out_specs=vmem,
        scratch_shapes=[
            pltpu.VMEM((depth, SIDE, count, width), kind),
            pltpu.VMEM((n, local + pad, count), jnp.float32),
            pltpu.VMEM((local, width, ff), kind),
            pltpu.VMEM((local, width, ff), kind),
            pltpu.VMEM((local * ff, width), kind),
            pltpu.VMEM((SIDE * count, local * ff), kind),
            pltpu.VMEM((depth, SIDE, count, width), kind),
            pltpu.VMEM((depth, count, width), kind),
            pltpu.VMEM((2, depth, SIDE, count, width), kind),
            dma((1 + 3 * local,)),
            dma((n,)), dma((n,)),
            dma((2, depth, SIDE, size)), dma((depth, SIDE, size)),
            dma((depth, size)), dma((depth, size)),
            dma((depth, size)), dma((depth, size)),
            dma((depth, SIDE, size)), dma((2, depth, SIDE, size)),
        ],
        compiler_params=pltpu.CompilerParams(
            collective_id=0, has_side_effects=True, vmem_limit_bytes=VMEM
        ),
    )(tokens, weights, w_gate, w_up, w_down)


def plain(tokens, expert_ids, gate_nums, w_gate, w_up, w_down, n):
    weight = expert_weights(expert_ids, gate_nums, w_gate.shape[0] * n)
    weights = lax.all_to_all(weight, "ep", split_axis=1, concat_axis=0, tiled=True)
    rows = lax.all_gather(tokens, "ep", axis=0, tiled=True)
    gate = jnp.einsum("td,xdf->xtf", rows, w_gate, preferred_element_type=jnp.float32)
    up = jnp.einsum("td,xdf->xtf", rows, w_up, preferred_element_type=jnp.float32)
    hidden = (jax.nn.silu(gate) * up * weights.T[:, :, None]).astype(jnp.bfloat16)
    result = jnp.einsum("xtf,xfd->td", hidden, w_down, preferred_element_type=jnp.float32)
    return lax.psum_scatter(
        result.astype(jnp.bfloat16), "ep", scatter_dimension=0, tiled=True
    )


def shards(n, tokens, expert_ids, gate_nums, w_gate, w_up, w_down):
    count, width = tokens.shape
    local, _, ff = w_gate.shape
    held = 5 * n * count * width + 3 * local * width * ff + 2 * count * local * ff
    fits = 2 * held < VMEM - 4 * 2**20
    shaped = n % (2 * SIDE) == 0 and count % 128 == 0 and ff % LANES == 0 and width % LANES == 0
    plan = fused if fits and shaped else plain
    return plan(tokens, expert_ids, gate_nums, w_gate, w_up, w_down, n)


def solution(mesh):
    placed = (
        P(("dp", "ep"), None),
        P(("dp", "ep"), None),
        P(("dp", "ep"), None),
        P("ep", None, None),
        P("ep", None, None),
        P("ep", None, None),
    )
    return jax.shard_map(
        functools.partial(shards, mesh.shape["ep"]),
        mesh=mesh, in_specs=placed, out_specs=P(("dp", "ep"), None), check_vma=False,
    )
```

```python
import functools

import jax
import jax.numpy as jnp
from jax import lax
from jax.experimental import pallas as pl
from jax.experimental.pallas import tpu as pltpu
from jax.sharding import PartitionSpec as P

denominator = 1024.0
SIDE = 2
LANES = 256
VMEM = 60 * 2**20


def expert_weights(expert_ids, gate_nums, experts):
    gates = gate_nums.astype(jnp.float32) / denominator
    labels = jnp.arange(experts, dtype=jnp.int32)
    onehot = expert_ids[:, :, None] == labels[None, None, :]
    return jnp.sum(jnp.where(onehot, gates[:, :, None], 0.0), axis=1)


def kernel(
    n, local, messages,
    tokens, weights, w_gate, w_up, w_down, out,
    rows, factors, gate, up, down, hidden, part, from_side, from_line,
    load_sem, weight_send, weight_recv, line_send, line_recv, side_send, side_recv,
    back_side_send, back_side_recv, back_line_send, back_line_recv,
):
    depth = n // SIDE
    me = lax.axis_index("ep")
    z, y = me // SIDE, me % SIDE
    other = SIDE - 1 - y
    partner = z * SIDE + other
    ff = w_gate.shape[2]
    count = tokens.shape[0]
    width = tokens.shape[1]
    last = depth - 1
    late = [m for m, (_, _, side, _) in enumerate(messages) if not side]
    early = [m for m, (_, _, side, _) in enumerate(messages) if side]
    late_back = [m for m, (_, _, _, side) in enumerate(messages) if not side]
    early_back = [m for m, (_, _, _, side) in enumerate(messages) if side]
    cuts = [pl.ds(start, size) for start, size, _, _ in messages]

    def remote(source, target, send, recv, device):
        return pltpu.make_async_remote_copy(
            src_ref=source, dst_ref=target, send_sem=send, recv_sem=recv,
            device_id={"ep": device}, device_id_type=pl.DeviceIdType.MESH,
        )

    own = pltpu.make_async_copy(tokens, rows.at[z, y], load_sem.at[0])
    own.start()
    loads = []
    for e in range(local):
        cut = pl.ds(e * ff, ff)
        loads.append(pltpu.make_async_copy(w_gate.at[e], gate.at[e], load_sem.at[1 + 3 * e]))
        loads.append(pltpu.make_async_copy(w_up.at[e], up.at[e], load_sem.at[2 + 3 * e]))
        loads.append(pltpu.make_async_copy(w_down.at[e], down.at[cut], load_sem.at[3 + 3 * e]))
    for load in loads:
        load.start()

    barrier = pltpu.get_barrier_semaphore()
    for k in range(1, n):
        pl.semaphore_signal(
            barrier, inc=1, device_id={"ep": (me + k) % n}, device_id_type=pl.DeviceIdType.MESH
        )
    pl.semaphore_wait(barrier, n - 1)
    own.wait()

    def side_copy(o, row, m):
        ref = rows.at[o, row, cuts[m]]
        return remote(ref, ref, side_send.at[o, m], side_recv.at[o, m], partner)

    def line_copy(o, row, m, way):
        ref = rows.at[o, row, cuts[m]]
        there = me + SIDE * (1 - 2 * way)
        return remote(
            ref, ref, line_send.at[way, o, row, m], line_recv.at[o, row, m], there
        )

    def onward(o, row, m, act):
        @pl.when((o <= z) & (z < last))
        def _():
            act(line_copy(o, row, m, 0))

        @pl.when((o >= z) & (z > 0))
        def _():
            act(line_copy(o, row, m, 1))

    def start(copy):
        copy.start()

    def wait_send(copy):
        copy.wait_send()

    def weight_copy(k):
        there = (me + k) % n
        return remote(weights.at[there], factors.at[me], weight_send.at[k], weight_recv.at[me], there)

    def back_side(o, m):
        return remote(
            part.at[o, other, cuts[m]], from_side.at[o, cuts[m]],
            back_side_send.at[o, m], back_side_recv.at[o, m], partner,
        )

    def back_line(o, row, m, way):
        there = me + SIDE * (1 - 2 * way)
        return remote(
            part.at[o, row, cuts[m]], from_line.at[way, o, row, cuts[m]],
            back_line_send.at[o, row, m], back_line_recv.at[way, o, row, m], there,
        )

    def each_back(o, row, m, act):
        @pl.when(o > z)
        def _():
            act(back_line(o, row, m, 0))

        @pl.when(o < z)
        def _():
            act(back_line(o, row, m, 1))

    for m in early:
        side_copy(z, y, m).start()
    for k in range(1, n):
        weight_copy(k).start()
    for m in late:
        onward(z, y, m, start)
        side_copy(z, y, m).start()
    for m in early:
        onward(z, y, m, start)
    factors[me] = weights[me]

    @pl.when(z == 0)
    def _():
        from_line[0] = jnp.zeros_like(from_line[0])

    @pl.when(z == last)
    def _():
        from_line[1] = jnp.zeros_like(from_line[1])

    for m in early:
        side_copy(z, other, m).wait_recv()
        onward(z, other, m, start)

    turn = 1 - 2 * (z // (depth // 2))
    pairs = jnp.minimum(z, last - z)
    middle = jnp.minimum(pairs, 1)

    def nearest(s):
        both = z + turn * ((s + 1) // 2) * (2 * (s % 2) - 1)
        single = z + turn * (s - pairs)
        return jnp.where(s <= 2 * pairs, both, single)

    def rotation(s):
        return (z + turn * s + depth) % depth

    def gather(o):
        for m in late:
            line_copy(o, y, m, 0).wait_recv()
            onward(o, y, m, start)
            side_copy(o, y, m).start()
        for m in early:
            for row in range(SIDE):
                line_copy(o, row, m, 0).wait_recv()
                onward(o, row, m, start)

    gather(nearest(1))

    @pl.when(middle == 1)
    def _():
        gather(nearest(2))

    for load in loads:
        load.wait()
    for k in range(1, n):
        source = (me + k) % n
        remote(
            factors.at[source], factors.at[source], weight_send.at[k], weight_recv.at[source], partner
        ).wait_recv()

    def arrive(o, row, m):
        @pl.when((o >= z) & (z > 0))
        def _():
            back_line(o, row, m, 0).wait_recv()

        @pl.when((o <= z) & (z < last))
        def _():
            back_line(o, row, m, 1).wait_recv()

    def wide(ref):
        return ref[...].astype(jnp.float32)

    def pass_back(o):
        way = (last + z - o) // depth
        for m in early_back:
            for row in range(SIDE):
                arrive(o, row, m)
                total = wide(part.at[o, row, cuts[m]]) + wide(from_line.at[way, o, row, cuts[m]])
                part[o, row, cuts[m]] = total.astype(part.dtype)
                each_back(o, row, m, start)
        for m in late_back:
            back_side(o, m).wait_recv()
            arrive(o, y, m)
            total = wide(part.at[o, y, cuts[m]]) + wide(from_line.at[way, o, y, cuts[m]])
            total = total + wide(from_side.at[o, cuts[m]])
            part[o, y, cuts[m]] = total.astype(part.dtype)
            each_back(o, y, m, start)

    def step(s, carry):
        o = nearest(s)
        for m in late:
            side_copy(o, other, m).wait_recv()
        scale = jnp.concatenate([factors[o * SIDE + i].T for i in range(SIDE)], axis=0)
        for e in range(local):
            column = scale[:, e : e + 1]

            def tile(t, carry):
                cut = pl.ds(pl.multiple_of(t * LANES, LANES), LANES)
                block = rows[o].reshape(SIDE * count, width)
                g = jnp.dot(block, gate[e, :, cut], preferred_element_type=jnp.float32)
                u = jnp.dot(block, up[e, :, cut], preferred_element_type=jnp.float32)
                h = g / (1.0 + jnp.exp(-g)) * u * column
                place = pl.ds(pl.multiple_of(e * ff + t * LANES, LANES), LANES)
                hidden[:, place] = h.astype(jnp.bfloat16)
                return carry

            lax.fori_loop(0, ff // LANES, tile, 0)

        def spread(t, carry):
            cut = pl.ds(pl.multiple_of(t * LANES, LANES), LANES)
            result = jnp.dot(hidden[...], down[:, cut], preferred_element_type=jnp.float32)
            part[o, :, :, cut] = result.astype(jnp.bfloat16).reshape(SIDE, count, LANES)
            return carry

        lax.fori_loop(0, width // LANES, spread, 0)

        @pl.when(s > 0)
        def _():
            for m in late_back:
                back_side(o, m).start()

        @pl.when(s + 2 + middle < depth)
        def _():
            gather(nearest(s + 2 + middle))

        @pl.when((s >= 2) & (middle == 0))
        def _():
            pass_back(rotation(s - 1))

        return carry

    lax.fori_loop(0, depth, step, 0)
    for m in late_back:
        back_side(z, m).start()

    def rest(s, carry):
        pass_back(rotation(s))
        return carry

    lax.fori_loop(1 + (1 - middle) * (depth - 2), depth, rest, 0)

    def collected(row, m):
        arrive(z, row, m)
        total = wide(part.at[z, row, cuts[m]])
        return total + wide(from_line.at[0, z, row, cuts[m]]) + wide(from_line.at[1, z, row, cuts[m]])

    for m in early_back:
        part[z, other, cuts[m]] = collected(other, m).astype(part.dtype)
        back_side(z, m).start()
    for m in late_back + early_back:
        total = collected(y, m)
        back_side(z, m).wait_recv()
        out[cuts[m]] = (total + wide(from_side.at[z, cuts[m]])).astype(out.dtype)

    for k in range(1, n):
        weight_copy(k).wait_send()
    for m in early:
        side_copy(z, y, m).wait_send()
    for m in early_back:
        back_side(z, m).wait_send()

    def settle(o, carry):
        for m in late:
            side_copy(o, y, m).wait_send()
            onward(o, y, m, wait_send)
        for m in late_back:
            back_side(o, m).wait_send()
            each_back(o, y, m, wait_send)
        for row in range(SIDE):
            for m in early:
                onward(o, row, m, wait_send)
            for m in early_back:
                each_back(o, row, m, wait_send)
        return carry

    lax.fori_loop(0, depth, settle, 0)


def fused(tokens, expert_ids, gate_nums, w_gate, w_up, w_down, n):
    count, width = tokens.shape
    local, _, ff = w_gate.shape
    depth = n // SIDE
    weight = expert_weights(expert_ids, gate_nums, local * n)
    pad = -local % 8
    weights = jnp.pad(weight.T.reshape(n, local, count), ((0, 0), (0, pad), (0, 0)))
    unit = count // 8
    messages = [(0 * unit, 2 * unit, False, False), (2 * unit, 2 * unit, False, False), (4 * unit, 3 * unit, False, False), (7 * unit, 1 * unit, True, False)]
    size = len(messages)
    kind = tokens.dtype
    dma = pltpu.SemaphoreType.DMA
    vmem = pl.BlockSpec(memory_space=pltpu.VMEM)
    hbm = pl.BlockSpec(memory_space=pl.ANY)
    return pl.pallas_call(
        functools.partial(kernel, n, local, messages),
        out_shape=jax.ShapeDtypeStruct((count, width), kind),
        in_specs=[hbm, vmem, hbm, hbm, hbm],
        out_specs=vmem,
        scratch_shapes=[
            pltpu.VMEM((depth, SIDE, count, width), kind),
            pltpu.VMEM((n, local + pad, count), jnp.float32),
            pltpu.VMEM((local, width, ff), kind),
            pltpu.VMEM((local, width, ff), kind),
            pltpu.VMEM((local * ff, width), kind),
            pltpu.VMEM((SIDE * count, local * ff), kind),
            pltpu.VMEM((depth, SIDE, count, width), kind),
            pltpu.VMEM((depth, count, width), kind),
            pltpu.VMEM((2, depth, SIDE, count, width), kind),
            dma((1 + 3 * local,)),
            dma((n,)), dma((n,)),
            dma((2, depth, SIDE, size)), dma((depth, SIDE, size)),
            dma((depth, size)), dma((depth, size)),
            dma((depth, size)), dma((depth, size)),
            dma((depth, SIDE, size)), dma((2, depth, SIDE, size)),
        ],
        compiler_params=pltpu.CompilerParams(
            collective_id=0, has_side_effects=True, vmem_limit_bytes=VMEM
        ),
    )(tokens, weights, w_gate, w_up, w_down)


def plain(tokens, expert_ids, gate_nums, w_gate, w_up, w_down, n):
    weight = expert_weights(expert_ids, gate_nums, w_gate.shape[0] * n)
    weights = lax.all_to_all(weight, "ep", split_axis=1, concat_axis=0, tiled=True)
    rows = lax.all_gather(tokens, "ep", axis=0, tiled=True)
    gate = jnp.einsum("td,xdf->xtf", rows, w_gate, preferred_element_type=jnp.float32)
    up = jnp.einsum("td,xdf->xtf", rows, w_up, preferred_element_type=jnp.float32)
    hidden = (jax.nn.silu(gate) * up * weights.T[:, :, None]).astype(jnp.bfloat16)
    result = jnp.einsum("xtf,xfd->td", hidden, w_down, preferred_element_type=jnp.float32)
    return lax.psum_scatter(
        result.astype(jnp.bfloat16), "ep", scatter_dimension=0, tiled=True
    )


def shards(n, tokens, expert_ids, gate_nums, w_gate, w_up, w_down):
    count, width = tokens.shape
    local, _, ff = w_gate.shape
    held = 5 * n * count * width + 3 * local * width * ff + 2 * count * local * ff
    fits = 2 * held < VMEM - 4 * 2**20
    shaped = n % (2 * SIDE) == 0 and count % 128 == 0 and ff % LANES == 0 and width % LANES == 0
    plan = fused if fits and shaped else plain
    return plan(tokens, expert_ids, gate_nums, w_gate, w_up, w_down, n)


def solution(mesh):
    placed = (
        P(("dp", "ep"), None),
        P(("dp", "ep"), None),
        P(("dp", "ep"), None),
        P("ep", None, None),
        P("ep", None, None),
        P("ep", None, None),
    )
    return jax.shard_map(
        functools.partial(shards, mesh.shape["ep"]),
        mesh=mesh, in_specs=placed, out_specs=P(("dp", "ep"), None), check_vma=False,
    )
```

```python
import functools

import jax
import jax.numpy as jnp
from jax import lax
from jax.experimental import pallas as pl
from jax.experimental.pallas import tpu as pltpu
from jax.sharding import PartitionSpec as P

denominator = 1024.0
SIDE = 2
LANES = 256
VMEM = 60 * 2**20


def expert_weights(expert_ids, gate_nums, experts):
    gates = gate_nums.astype(jnp.float32) / denominator
    labels = jnp.arange(experts, dtype=jnp.int32)
    onehot = expert_ids[:, :, None] == labels[None, None, :]
    return jnp.sum(jnp.where(onehot, gates[:, :, None], 0.0), axis=1)


def kernel(
    n, local, messages,
    tokens, weights, w_gate, w_up, w_down, out,
    rows, factors, gate, up, down, hidden, part, from_side, from_line,
    load_sem, weight_send, weight_recv, line_send, line_recv, side_send, side_recv,
    back_side_send, back_side_recv, back_line_send, back_line_recv,
):
    depth = n // SIDE
    me = lax.axis_index("ep")
    z, y = me // SIDE, me % SIDE
    other = SIDE - 1 - y
    partner = z * SIDE + other
    ff = w_gate.shape[2]
    count = tokens.shape[0]
    width = tokens.shape[1]
    last = depth - 1
    late = [m for m, (_, _, side, _) in enumerate(messages) if not side]
    early = [m for m, (_, _, side, _) in enumerate(messages) if side]
    late_back = [m for m, (_, _, _, side) in enumerate(messages) if not side]
    early_back = [m for m, (_, _, _, side) in enumerate(messages) if side]
    cuts = [pl.ds(start, size) for start, size, _, _ in messages]

    def remote(source, target, send, recv, device):
        return pltpu.make_async_remote_copy(
            src_ref=source, dst_ref=target, send_sem=send, recv_sem=recv,
            device_id={"ep": device}, device_id_type=pl.DeviceIdType.MESH,
        )

    own = pltpu.make_async_copy(tokens, rows.at[z, y], load_sem.at[0])
    own.start()
    loads = []
    for e in range(local):
        cut = pl.ds(e * ff, ff)
        loads.append(pltpu.make_async_copy(w_gate.at[e], gate.at[e], load_sem.at[1 + 3 * e]))
        loads.append(pltpu.make_async_copy(w_up.at[e], up.at[e], load_sem.at[2 + 3 * e]))
        loads.append(pltpu.make_async_copy(w_down.at[e], down.at[cut], load_sem.at[3 + 3 * e]))
    for load in loads:
        load.start()

    barrier = pltpu.get_barrier_semaphore()
    for k in range(1, n):
        pl.semaphore_signal(
            barrier, inc=1, device_id={"ep": (me + k) % n}, device_id_type=pl.DeviceIdType.MESH
        )
    pl.semaphore_wait(barrier, n - 1)
    own.wait()

    def side_copy(o, row, m):
        ref = rows.at[o, row, cuts[m]]
        return remote(ref, ref, side_send.at[o, m], side_recv.at[o, m], partner)

    def line_copy(o, row, m, way):
        ref = rows.at[o, row, cuts[m]]
        there = me + SIDE * (1 - 2 * way)
        return remote(
            ref, ref, line_send.at[way, o, row, m], line_recv.at[o, row, m], there
        )

    def onward(o, row, m, act):
        @pl.when((o <= z) & (z < last))
        def _():
            act(line_copy(o, row, m, 0))

        @pl.when((o >= z) & (z > 0))
        def _():
            act(line_copy(o, row, m, 1))

    def start(copy):
        copy.start()

    def wait_send(copy):
        copy.wait_send()

    def weight_copy(k):
        there = (me + k) % n
        return remote(weights.at[there], factors.at[me], weight_send.at[k], weight_recv.at[me], there)

    def back_side(o, m):
        return remote(
            part.at[o, other, cuts[m]], from_side.at[o, cuts[m]],
            back_side_send.at[o, m], back_side_recv.at[o, m], partner,
        )

    def back_line(o, row, m, way):
        there = me + SIDE * (1 - 2 * way)
        return remote(
            part.at[o, row, cuts[m]], from_line.at[way, o, row, cuts[m]],
            back_line_send.at[o, row, m], back_line_recv.at[way, o, row, m], there,
        )

    def each_back(o, row, m, act):
        @pl.when(o > z)
        def _():
            act(back_line(o, row, m, 0))

        @pl.when(o < z)
        def _():
            act(back_line(o, row, m, 1))

    for m in early:
        side_copy(z, y, m).start()
    for k in range(1, n):
        weight_copy(k).start()
    for m in late:
        onward(z, y, m, start)
        side_copy(z, y, m).start()
    for m in early:
        onward(z, y, m, start)
    factors[me] = weights[me]

    @pl.when(z == 0)
    def _():
        from_line[0] = jnp.zeros_like(from_line[0])

    @pl.when(z == last)
    def _():
        from_line[1] = jnp.zeros_like(from_line[1])

    for m in early:
        side_copy(z, other, m).wait_recv()
        onward(z, other, m, start)

    turn = 1 - 2 * (z // (depth // 2))
    pairs = jnp.minimum(z, last - z)
    middle = jnp.minimum(pairs, 1)

    def nearest(s):
        both = z + turn * ((s + 1) // 2) * (2 * (s % 2) - 1)
        single = z + turn * (s - pairs)
        return jnp.where(s <= 2 * pairs, both, single)

    def rotation(s):
        return (z + turn * s + depth) % depth

    def gather(o):
        for m in late:
            line_copy(o, y, m, 0).wait_recv()
            onward(o, y, m, start)
            side_copy(o, y, m).start()
        for m in early:
            for row in range(SIDE):
                line_copy(o, row, m, 0).wait_recv()
                onward(o, row, m, start)

    gather(nearest(1))

    @pl.when(middle == 1)
    def _():
        gather(nearest(2))

    for load in loads:
        load.wait()
    for k in range(1, n):
        source = (me + k) % n
        remote(
            factors.at[source], factors.at[source], weight_send.at[k], weight_recv.at[source], partner
        ).wait_recv()

    def arrive(o, row, m):
        @pl.when((o >= z) & (z > 0))
        def _():
            back_line(o, row, m, 0).wait_recv()

        @pl.when((o <= z) & (z < last))
        def _():
            back_line(o, row, m, 1).wait_recv()

    def wide(ref):
        return ref[...].astype(jnp.float32)

    def pass_back(o):
        way = (last + z - o) // depth
        for m in early_back:
            for row in range(SIDE):
                arrive(o, row, m)
                total = wide(part.at[o, row, cuts[m]]) + wide(from_line.at[way, o, row, cuts[m]])
                part[o, row, cuts[m]] = total.astype(part.dtype)
                each_back(o, row, m, start)
        for m in late_back:
            back_side(o, m).wait_recv()
            arrive(o, y, m)
            total = wide(part.at[o, y, cuts[m]]) + wide(from_line.at[way, o, y, cuts[m]])
            total = total + wide(from_side.at[o, cuts[m]])
            part[o, y, cuts[m]] = total.astype(part.dtype)
            each_back(o, y, m, start)

    def step(s, carry):
        o = nearest(s)
        for m in late:
            side_copy(o, other, m).wait_recv()
        scale = jnp.concatenate([factors[o * SIDE + i].T for i in range(SIDE)], axis=0)
        for e in range(local):
            column = scale[:, e : e + 1]

            def tile(t, carry):
                cut = pl.ds(pl.multiple_of(t * LANES, LANES), LANES)
                block = rows[o].reshape(SIDE * count, width)
                g = jnp.dot(block, gate[e, :, cut], preferred_element_type=jnp.float32)
                u = jnp.dot(block, up[e, :, cut], preferred_element_type=jnp.float32)
                h = g / (1.0 + jnp.exp(-g)) * u * column
                place = pl.ds(pl.multiple_of(e * ff + t * LANES, LANES), LANES)
                hidden[:, place] = h.astype(jnp.bfloat16)
                return carry

            lax.fori_loop(0, ff // LANES, tile, 0, unroll=True)

        def spread(t, carry):
            cut = pl.ds(pl.multiple_of(t * LANES, LANES), LANES)
            result = jnp.dot(hidden[...], down[:, cut], preferred_element_type=jnp.float32)
            part[o, :, :, cut] = result.astype(jnp.bfloat16).reshape(SIDE, count, LANES)
            return carry

        lax.fori_loop(0, width // LANES, spread, 0, unroll=True)

        @pl.when(s > 0)
        def _():
            for m in late_back:
                back_side(o, m).start()

        @pl.when(s + 2 + middle < depth)
        def _():
            gather(nearest(s + 2 + middle))

        @pl.when((s >= 2) & (middle == 0))
        def _():
            pass_back(rotation(s - 1))

        return carry

    lax.fori_loop(0, depth, step, 0)
    for m in late_back:
        back_side(z, m).start()

    def rest(s, carry):
        pass_back(rotation(s))
        return carry

    lax.fori_loop(1 + (1 - middle) * (depth - 2), depth, rest, 0)

    def collected(row, m):
        arrive(z, row, m)
        total = wide(part.at[z, row, cuts[m]])
        return total + wide(from_line.at[0, z, row, cuts[m]]) + wide(from_line.at[1, z, row, cuts[m]])

    for m in early_back:
        part[z, other, cuts[m]] = collected(other, m).astype(part.dtype)
        back_side(z, m).start()
    for m in late_back + early_back:
        total = collected(y, m)
        back_side(z, m).wait_recv()
        out[cuts[m]] = (total + wide(from_side.at[z, cuts[m]])).astype(out.dtype)

    for k in range(1, n):
        weight_copy(k).wait_send()
    for m in early:
        side_copy(z, y, m).wait_send()
    for m in early_back:
        back_side(z, m).wait_send()

    def settle(o, carry):
        for m in late:
            side_copy(o, y, m).wait_send()
            onward(o, y, m, wait_send)
        for m in late_back:
            back_side(o, m).wait_send()
            each_back(o, y, m, wait_send)
        for row in range(SIDE):
            for m in early:
                onward(o, row, m, wait_send)
            for m in early_back:
                each_back(o, row, m, wait_send)
        return carry

    lax.fori_loop(0, depth, settle, 0)


def fused(tokens, expert_ids, gate_nums, w_gate, w_up, w_down, n):
    count, width = tokens.shape
    local, _, ff = w_gate.shape
    depth = n // SIDE
    weight = expert_weights(expert_ids, gate_nums, local * n)
    pad = -local % 8
    weights = jnp.pad(weight.T.reshape(n, local, count), ((0, 0), (0, pad), (0, 0)))
    unit = count // 8
    messages = [(0 * unit, 2 * unit, False, False), (2 * unit, 2 * unit, False, False), (4 * unit, 2 * unit, False, False), (6 * unit, 1 * unit, False, False), (7 * unit, 1 * unit, True, False)]
    size = len(messages)
    kind = tokens.dtype
    dma = pltpu.SemaphoreType.DMA
    vmem = pl.BlockSpec(memory_space=pltpu.VMEM)
    hbm = pl.BlockSpec(memory_space=pl.ANY)
    return pl.pallas_call(
        functools.partial(kernel, n, local, messages),
        out_shape=jax.ShapeDtypeStruct((count, width), kind),
        in_specs=[hbm, vmem, hbm, hbm, hbm],
        out_specs=vmem,
        scratch_shapes=[
            pltpu.VMEM((depth, SIDE, count, width), kind),
            pltpu.VMEM((n, local + pad, count), jnp.float32),
            pltpu.VMEM((local, width, ff), kind),
            pltpu.VMEM((local, width, ff), kind),
            pltpu.VMEM((local * ff, width), kind),
            pltpu.VMEM((SIDE * count, local * ff), kind),
            pltpu.VMEM((depth, SIDE, count, width), kind),
            pltpu.VMEM((depth, count, width), kind),
            pltpu.VMEM((2, depth, SIDE, count, width), kind),
            dma((1 + 3 * local,)),
            dma((n,)), dma((n,)),
            dma((2, depth, SIDE, size)), dma((depth, SIDE, size)),
            dma((depth, size)), dma((depth, size)),
            dma((depth, size)), dma((depth, size)),
            dma((depth, SIDE, size)), dma((2, depth, SIDE, size)),
        ],
        compiler_params=pltpu.CompilerParams(
            collective_id=0, has_side_effects=True, vmem_limit_bytes=VMEM
        ),
    )(tokens, weights, w_gate, w_up, w_down)


def plain(tokens, expert_ids, gate_nums, w_gate, w_up, w_down, n):
    weight = expert_weights(expert_ids, gate_nums, w_gate.shape[0] * n)
    weights = lax.all_to_all(weight, "ep", split_axis=1, concat_axis=0, tiled=True)
    rows = lax.all_gather(tokens, "ep", axis=0, tiled=True)
    gate = jnp.einsum("td,xdf->xtf", rows, w_gate, preferred_element_type=jnp.float32)
    up = jnp.einsum("td,xdf->xtf", rows, w_up, preferred_element_type=jnp.float32)
    hidden = (jax.nn.silu(gate) * up * weights.T[:, :, None]).astype(jnp.bfloat16)
    result = jnp.einsum("xtf,xfd->td", hidden, w_down, preferred_element_type=jnp.float32)
    return lax.psum_scatter(
        result.astype(jnp.bfloat16), "ep", scatter_dimension=0, tiled=True
    )


def shards(n, tokens, expert_ids, gate_nums, w_gate, w_up, w_down):
    count, width = tokens.shape
    local, _, ff = w_gate.shape
    held = 5 * n * count * width + 3 * local * width * ff + 2 * count * local * ff
    fits = 2 * held < VMEM - 4 * 2**20
    shaped = n % (2 * SIDE) == 0 and count % 128 == 0 and ff % LANES == 0 and width % LANES == 0
    plan = fused if fits and shaped else plain
    return plan(tokens, expert_ids, gate_nums, w_gate, w_up, w_down, n)


def solution(mesh):
    placed = (
        P(("dp", "ep"), None),
        P(("dp", "ep"), None),
        P(("dp", "ep"), None),
        P("ep", None, None),
        P("ep", None, None),
        P("ep", None, None),
    )
    return jax.shard_map(
        functools.partial(shards, mesh.shape["ep"]),
        mesh=mesh, in_specs=placed, out_specs=P(("dp", "ep"), None), check_vma=False,
    )
```
